32 devices in a mesh: fft: 16 (over z, x, core), scal: 2 (over y).
Axes of the slice: x: 2, y: 2, z: 4, core: 2. Of those that a mesh axis runs over, the one named last changes fastest.
Arguments:
- scalar_state: float32 [2, 2, 256, 256, 128], P('scal', None, 'fft'), may hold values from -12 to 12
- velocity: bfloat16 [3, 256, 256, 256], P(None, 'fft', 'scal'), may hold values from -6 to 6
- species: int32 [2], P('scal'), may hold values from 0 to 63
- kappa_table: float32 [64], replicated, may hold values from 0.1 to 1
- dealias_bound: int32 [2], P('scal'), may hold values from 64 to 85
Outputs:
- new_state: float32 [2, 2, 256, 256, 128], P('scal', None, 'fft')
- kappa: float32 [2], P('scal')
The draws below stay inside these ranges and needn't reach their ends.
All inputs are finite; a program needn't handle non-finite values.
Results may differ from the reference program's by a relative error of at most 0.0027.
Values may be sent and summed in bfloat16 or wider, within the bound.
A program may use at most 128 MiB of HBM per device.

```python
import math
import jax
import jax.numpy as jnp
from jax import lax

N = 256
SPECIES = 64
SCALARS = 2


def draw_scalar_state(key, part):
    dims_shape = (SCALARS, 2, N, N, N // 2)
    key_base, key_rough, key_scale = jax.random.split(key, 3)
    values = jnp.clip(jax.random.normal(key_base, dims_shape, jnp.float32), -4.0, 4.0)
    roughness = jnp.exp(jax.random.uniform(key_rough, dims_shape, jnp.float32, math.log(0.5), math.log(1.5)))
    ky_float = jnp.arange(N, dtype=jnp.int32).astype(jnp.float32)
    envelope = jnp.sqrt(1.0 + 2.0 * ky_float / (N - 1)).reshape(1, 1, N, 1, 1)
    scalar_scale = jnp.exp(jax.random.uniform(key_scale, (SCALARS, 1, 1, 1, 1), jnp.float32, math.log(0.5), math.log(2.0)))
    return jnp.clip(values * roughness * envelope * scalar_scale, -12.0, 12.0).astype(jnp.float32)


def block_scale(rng, dims, cuts, least, largest):
    loudness, own = 1.0, jax.random.fold_in(rng, 6)
    for position, shards_of in cuts:
        heights = jnp.exp(jax.random.uniform(jax.random.fold_in(own, position), (shards_of,), jnp.float32, least / len(cuts), largest / len(cuts)))
        loudness = loudness * jnp.repeat(heights, dims[position] // shards_of).reshape([-1 if axis == position else 1 for axis in range(len(dims))])
    return loudness


def noise(stream_key, shape, spread, most, cuts=(), kind=jnp.bfloat16):
    entries = jax.random.normal(stream_key, shape, jnp.float32) * spread
    if len(cuts) > 0:
        entries = block_scale(stream_key, shape, cuts, -0.22, 0.18) * entries
    return jnp.clip(entries, min=-most, max=most).astype(kind)


def setup_inputs(seed: int = 0) -> dict:
    keys = jax.random.split(jax.random.key(seed), 6)
    return {
        "scalar_state": draw_scalar_state(jax.random.fold_in(keys[5], 71), 0),
        "velocity": noise(keys[1], (3, N, N, N), 1.0, 6.0, ((1, 16), (2, 2))),
        "species": jax.random.randint(keys[2], (SCALARS,), 0, SPECIES).astype(jnp.int32),
        "kappa_table": jnp.clip(jnp.exp(jax.random.uniform(keys[3], (SPECIES,), jnp.float32, math.log(0.1), math.log(1.0))), 0.1, 1.0),
        "dealias_bound": jax.random.randint(keys[4], (SCALARS,), N // 4, N // 3 + 1).astype(jnp.int32),
    }


cfl_number = 0.2

def twiddle(size_in, size_out, length):
    row_index = jnp.arange(size_in, dtype=jnp.int32)[:, None]
    col_index = jnp.arange(size_out, dtype=jnp.int32)[None, :]
    angles = (row_index * col_index % length).astype(jnp.float32) * (2.0 * math.pi / length)
    norming = 1.0 / math.sqrt(length)
    return (jnp.cos(angles) * norming, jnp.sin(angles) * norming)

def build_tables(length):
    half_len = length // 2
    full_cos, full_sin = twiddle(length, length, length)
    inv_cos, inv_sin = twiddle(half_len, length, length)
    weight = jnp.where(jnp.arange(half_len, dtype=jnp.int32) == 0, 1.0, 2.0).astype(jnp.float32)[:, None]
    fwd_cos, fwd_sin = twiddle(length, half_len, length)
    listed = (full_cos, full_sin, inv_cos * weight, inv_sin * weight, fwd_cos, fwd_sin)
    return tuple((matrix.astype(jnp.bfloat16) for matrix in listed))

def product(formula, operand, matrix):
    return jnp.einsum(formula, operand.astype(jnp.float32), matrix.astype(jnp.float32), precision=lax.Precision.HIGHEST)

def complex_section(real_part, imag_part, cos_matrix, sin_matrix, formula, inverse):
    real_cos = product(formula, real_part, cos_matrix)
    real_sin = product(formula, real_part, sin_matrix)
    imag_cos = product(formula, imag_part, cos_matrix)
    imag_sin = product(formula, imag_part, sin_matrix)
    if inverse:
        return (real_cos - imag_sin, real_sin + imag_cos)
    return (real_cos + imag_sin, imag_cos - real_sin)

def reference(scalar_state, velocity, species, kappa_table, dealias_bound):
    scalar_count = scalar_state.shape[0]
    table_count = kappa_table.shape[0]
    length = scalar_state.shape[2]
    half_len = length // 2
    full_cos, full_sin, inv_cos, inv_sin, fwd_cos, fwd_sin = build_tables(length)
    index_full = jnp.arange(length, dtype=jnp.int32)
    signed = jnp.where(index_full < half_len, index_full, index_full - length).astype(jnp.float32)
    ky_wave = signed[:, None, None]
    kz_wave = signed[None, :, None]
    kx_wave = jnp.arange(half_len, dtype=jnp.int32).astype(jnp.float32)[None, None, :]
    ksquare = kx_wave * kx_wave + ky_wave * ky_wave + kz_wave * kz_wave
    weight = jnp.where(kx_wave == 0.0, 1.0, 2.0).astype(jnp.float32)
    cell_count = float(length) ** 3
    step_size = cfl_number * 2.0 * math.pi / length

    def z_inverse(real_part, imag_part):
        z_section = complex_section(real_part, imag_part, full_cos, full_sin, 'ykx,kz->yzx', True)
        return (z_section[0].astype(jnp.bfloat16), z_section[1].astype(jnp.bfloat16))

    def rest_inverse(real_part, imag_part):
        y_section = complex_section(real_part, imag_part, full_cos, full_sin, 'yzx,yw->zwx', True)
        y_real = y_section[0].astype(jnp.bfloat16)
        y_imag = y_section[1].astype(jnp.bfloat16)
        return product('zwk,kx->zwx', y_real, inv_cos) - product('zwk,kx->zwx', y_imag, inv_sin)

    def gradient_set(real_part, imag_part):
        whole_real, whole_imag = z_inverse(real_part.astype(jnp.bfloat16), imag_part.astype(jnp.bfloat16))
        deriv_real, deriv_imag = z_inverse((-kz_wave * imag_part).astype(jnp.bfloat16), (kz_wave * real_part).astype(jnp.bfloat16))
        results = []
        for wavenumber in (kx_wave, ky_wave):
            grad_real = (-wavenumber * whole_imag.astype(jnp.float32)).astype(jnp.bfloat16)
            grad_imag = (wavenumber * whole_real.astype(jnp.float32)).astype(jnp.bfloat16)
            results.append(rest_inverse(grad_real, grad_imag))
        results.append(rest_inverse(deriv_real, deriv_imag))
        return results

    def advect(gradients):
        total = velocity[0].astype(jnp.float32) * gradients[0]
        total = total + velocity[1].astype(jnp.float32) * gradients[1]
        total = total + velocity[2].astype(jnp.float32) * gradients[2]
        return total.astype(jnp.bfloat16)

    def forward_field(physical):
        real_x = product('zyx,xk->zyk', physical, fwd_cos).astype(jnp.bfloat16)
        imag_x = (-product('zyx,xk->zyk', physical, fwd_sin)).astype(jnp.bfloat16)
        y_section = complex_section(real_x, imag_x, full_cos, full_sin, 'zyk,yw->wzk', False)
        y_real = y_section[0].astype(jnp.bfloat16)
        y_imag = y_section[1].astype(jnp.bfloat16)
        return complex_section(y_real, y_imag, full_cos, full_sin, 'wzk,zv->wvk', False)
    updated_list = []
    kappa_list = []
    for scalar in range(scalar_count):
        start_real = scalar_state[scalar, 0]
        start_imag = scalar_state[scalar, 1]
        energy = start_real * start_real + start_imag * start_imag
        variance = jnp.sum(weight * energy) / cell_count
        mean_grad = jnp.sum(weight * ksquare * energy) / cell_count
        gradients = gradient_set(start_real, start_imag)
        peak_value = jnp.max(jnp.sqrt(gradients[0] * gradients[0] + gradients[1] * gradients[1] + gradients[2] * gradients[2]))
        base_kappa = jnp.sum(jnp.where(species[scalar] == jnp.arange(table_count, dtype=jnp.int32), kappa_table, 0.0))
        kappa_value = base_kappa * peak_value * jnp.sqrt(variance) / (mean_grad + 1e-06)
        factor = jnp.exp(-kappa_value * ksquare * step_size)
        bound = dealias_bound[scalar].astype(jnp.float32)
        dealias_mask = (ksquare <= bound * bound).astype(jnp.float32)
        first_real, first_imag = forward_field(advect(gradients))
        first_real = -dealias_mask * first_real
        first_imag = -dealias_mask * first_imag
        mid_real = factor * (start_real + step_size * first_real)
        mid_imag = factor * (start_imag + step_size * first_imag)
        second_real, second_imag = forward_field(advect(gradient_set(mid_real, mid_imag)))
        second_real = -dealias_mask * second_real
        second_imag = -dealias_mask * second_imag
        new_real = factor * start_real + 0.5 * step_size * (factor * first_real + second_real)
        new_imag = factor * start_imag + 0.5 * step_size * (factor * first_imag + second_imag)
        updated_list.append(jnp.stack([new_real, new_imag]))
        kappa_list.append(kappa_value)
    return (jnp.stack(updated_list), jnp.stack(kappa_list))
```

```python
import functools
import math

import jax
import jax.numpy as jnp
from jax import lax
from jax.experimental import pallas as pl
from jax.experimental.pallas import tpu as pltpu
from jax.sharding import PartitionSpec as P

MESH = pl.DeviceIdType.MESH
cfl_number = 0.2


def twiddle(size_in, size_out, length):
    row_index = jnp.arange(size_in, dtype=jnp.int32)[:, None]
    col_index = jnp.arange(size_out, dtype=jnp.int32)[None, :]
    angles = (row_index * col_index % length).astype(jnp.float32) * (2.0 * math.pi / length)
    norming = 1.0 / math.sqrt(length)
    return (jnp.cos(angles) * norming, jnp.sin(angles) * norming)


def build_tables(length):
    half_len = length // 2
    full_cos, full_sin = twiddle(length, length, length)
    inv_cos, inv_sin = twiddle(half_len, length, length)
    weight = jnp.where(jnp.arange(half_len, dtype=jnp.int32) == 0, 1.0, 2.0).astype(jnp.float32)[
        :, None
    ]
    fwd_cos, fwd_sin = twiddle(length, half_len, length)
    listed = (full_cos, full_sin, inv_cos * weight, inv_sin * weight, fwd_cos, fwd_sin)
    return tuple((matrix.astype(jnp.bfloat16) for matrix in listed))


def dot(a, b):
    return jnp.dot(a, b, preferred_element_type=jnp.float32)


def stage_kernel(n, m, rows, chunk, band, first, *refs):
    if first:
        (send, vel, stat_in, inv_y, inv_x, fwd_x, fwd_y,
         gout, uall, stat_out,
         recv, fsend, peak, stat, s_send, s_recv, f_send, f_recv, l_sem, u_send, u_recv, u_loc,
         t_send, t_recv, t_loc) = refs
    else:
        (send, uall, inv_y, inv_x, fwd_x, fwd_y,
         gout,
         recv, fsend, s_send, s_recv, f_send, f_recv, l_sem) = refs
    length = n * rows
    half = length // 2
    count = rows // chunk
    me = lax.axis_index("fft")
    mine = lax.axis_index("scal")

    def inside(d):
        return jnp.logical_or(d * rows <= band, (d + 1) * rows - 1 >= length - band)

    barrier = pltpu.get_barrier_semaphore()

    def greet(j, carry):
        pl.semaphore_signal(barrier, inc=1, device_id={"fft": lax.rem(me + j, n)}, device_id_type=MESH)
        return carry

    lax.fori_loop(1, n, greet, 0)
    if first:
        def greet_other(j, carry):
            pl.semaphore_signal(
                barrier, inc=1, device_id={"scal": lax.rem(mine + j, m)}, device_id_type=MESH
            )
            return carry

        lax.fori_loop(1, m, greet_other, 0)
        pl.semaphore_wait(barrier, n + m - 2)
    else:
        pl.semaphore_wait(barrier, n - 1)

    def inverse_copy(c, d, slot):
        return pltpu.make_async_remote_copy(
            src_ref=send.at[d, pl.ds(c * chunk, chunk)],
            dst_ref=recv.at[pl.ds(c * chunk, chunk), :, slot],
            send_sem=s_send.at[c, d],
            recv_sem=s_recv.at[c, slot],
            device_id={"fft": d},
            device_id_type=MESH,
        )

    def own_copy(c):
        return pltpu.make_async_copy(
            send.at[me, pl.ds(c * chunk, chunk)], recv.at[pl.ds(c * chunk, chunk), :, me], l_sem.at[0, c]
        )

    def speed_copy(c, s, slot):
        return pltpu.make_async_remote_copy(
            src_ref=vel.at[:, pl.ds(c * chunk, chunk)],
            dst_ref=uall.at[:, pl.ds(c * chunk, chunk), slot],
            send_sem=u_send.at[c, s],
            recv_sem=u_recv.at[c, slot],
            device_id={"scal": s},
            device_id_type=MESH,
        )

    def own_speed(c):
        return pltpu.make_async_copy(
            vel.at[:, pl.ds(c * chunk, chunk)], uall.at[:, pl.ds(c * chunk, chunk), mine], u_loc.at[c]
        )

    def forward_copy(c, d, slot):
        return pltpu.make_async_remote_copy(
            src_ref=fsend.at[d, pl.ds(c * chunk, chunk)],
            dst_ref=gout.at[slot, pl.ds(c * chunk, chunk)],
            send_sem=f_send.at[c, d],
            recv_sem=f_recv.at[c, slot],
            device_id={"fft": d},
            device_id_type=MESH,
        )

    def own_forward(c):
        return pltpu.make_async_copy(
            fsend.at[me, pl.ds(c * chunk, chunk)], gout.at[me, pl.ds(c * chunk, chunk)], l_sem.at[1, c]
        )

    def stat_copy(d, slot):
        return pltpu.make_async_remote_copy(
            src_ref=stat,
            dst_ref=stat_out.at[slot],
            send_sem=t_send.at[d],
            recv_sem=t_recv.at[slot],
            device_id={"fft": d},
            device_id_type=MESH,
        )

    def start_chunk(c, carry):
        def one(j, inner):
            inverse_copy(c, lax.rem(me + j, n), me).start()
            return inner

        lax.fori_loop(1, n, one, 0)
        own_copy(c).start()
        if first:
            def two(j, inner):
                speed_copy(c, lax.rem(mine + j, m), mine).start()
                return inner

            lax.fori_loop(1, m, two, 0)
            own_speed(c).start()
        return carry

    lax.fori_loop(0, count, start_chunk, 0)

    if first:
        peak[...] = jnp.zeros_like(peak)

    @pl.when(jnp.logical_not(inside(me)))
    def _():
        gout[...] = jnp.zeros_like(gout)

    row = lax.broadcasted_iota(jnp.int32, (length, half), 0)
    ky = jnp.where(row < half, row, row - length).astype(jnp.float32)
    kx = lax.broadcasted_iota(jnp.int32, (length, half), 1).astype(jnp.float32)

    def pair(z):
        parts = []
        for p in range(2):
            block = recv[z + p].reshape(2 * length, 2 * half)
            w_real = block[:length, :half].astype(jnp.float32)
            w_imag = block[length:, :half].astype(jnp.float32)
            turned = jnp.concatenate(
                [(-ky * w_imag).astype(jnp.bfloat16), (ky * w_real).astype(jnp.bfloat16)], axis=0
            )
            parts += [block, turned]
        section = dot(inv_y[...], jnp.concatenate(parts, axis=1))
        halves = []
        for p in range(2):
            at = 3 * half * p
            w_real = section[:length, at : at + half]
            w_imag = section[length:, at : at + half]
            sides = [
                (-kx * w_imag, kx * w_real),
                (section[:length, at + 2 * half : at + 3 * half], section[length:, at + 2 * half : at + 3 * half]),
                (section[:length, at + half : at + 2 * half], section[length:, at + half : at + 2 * half]),
            ]
            total = None
            square = None
            for i, (re, im) in enumerate(sides):
                lhs = jnp.concatenate([re.astype(jnp.bfloat16), im.astype(jnp.bfloat16)], axis=1)
                grad = dot(lhs, inv_x[...])
                u = uall[i, z + p].reshape(length, length).astype(jnp.float32)
                total = u * grad if total is None else total + u * grad
                if first:
                    square = grad * grad if square is None else square + grad * grad
            if first:
                peak[...] = jnp.maximum(peak[...], jnp.max(square.reshape(length // 8, 8, length), axis=0))
            flat = dot(total.astype(jnp.bfloat16), fwd_x[...]).astype(jnp.bfloat16)
            halves.append(jnp.concatenate([flat[:, :half], flat[:, half:]], axis=0))
        out = dot(fwd_y[...], jnp.concatenate(halves, axis=1)).astype(jnp.bfloat16)
        for p in range(2):
            for q in range(2):
                fsend[:, z + p, q] = out[q * length : (q + 1) * length, p * half : (p + 1) * half].reshape(
                    n, rows, half
                )

    def run_chunk(c, carry):
        def arrive(j, inner):
            inverse_copy(c, lax.rem(me + j, n), lax.rem(me + n - j, n)).wait_recv()
            return inner

        lax.fori_loop(1, n, arrive, 0)
        own_copy(c).wait()
        if first:
            def arrive_speed(j, inner):
                speed_copy(c, lax.rem(mine + j, m), lax.rem(mine + m - j, m)).wait_recv()
                return inner

            lax.fori_loop(1, m, arrive_speed, 0)
            own_speed(c).wait()

        def one(i, inner):
            pair(c * chunk + 2 * i)
            return inner

        lax.fori_loop(0, chunk // 2, one, 0)

        def leave(j, inner):
            d = lax.rem(me + j, n)

            @pl.when(inside(d))
            def _():
                forward_copy(c, d, me).start()

            return inner

        lax.fori_loop(1, n, leave, 0)

        @pl.when(inside(me))
        def _():
            own_forward(c).start()

        return carry

    lax.fori_loop(0, count, run_chunk, 0)

    if first:
        line = lax.broadcasted_iota(jnp.int32, stat.shape, 0)
        largest = jnp.sqrt(jnp.max(peak[...], keepdims=True))
        stat[...] = jnp.where(line == 2, largest, stat_in[...])

        def tell(j, carry):
            stat_copy(lax.rem(me + j, n), me).start()
            return carry

        lax.fori_loop(1, n, tell, 0)
        pltpu.make_async_copy(stat, stat_out.at[me], t_loc).start()

    def finish(c, carry):
        def one(j, inner):
            d = lax.rem(me + j, n)
            inverse_copy(c, d, me).wait_send()

            @pl.when(inside(d))
            def _():
                forward_copy(c, d, me).wait_send()

            @pl.when(inside(me))
            def _():
                forward_copy(c, d, lax.rem(me + n - j, n)).wait_recv()

            return inner

        lax.fori_loop(1, n, one, 0)

        @pl.when(inside(me))
        def _():
            own_forward(c).wait()

        if first:
            def two(j, inner):
                speed_copy(c, lax.rem(mine + j, m), mine).wait_send()
                return inner

            lax.fori_loop(1, m, two, 0)
        return carry

    lax.fori_loop(0, count, finish, 0)

    if first:
        def told(j, carry):
            stat_copy(lax.rem(me + j, n), me).wait_send()
            stat_copy(lax.rem(me + j, n), lax.rem(me + n - j, n)).wait_recv()
            return carry

        lax.fori_loop(1, n, told, 0)
        pltpu.make_async_copy(stat, stat_out.at[me], t_loc).wait()


def run_stage(n, m, rows, first, send, speeds, tables, stat_in=None):
    length = n * rows
    half = length // 2
    chunk = max(2, rows // 4)
    count = rows // chunk
    band = length // 3
    vmem = pl.BlockSpec(memory_space=pltpu.VMEM)
    hbm = pl.BlockSpec(memory_space=pl.ANY)
    dma = pltpu.SemaphoreType.DMA
    out_shape = [jax.ShapeDtypeStruct((n, rows, 2, rows, half), jnp.bfloat16)]
    scratch = [
        pltpu.VMEM((rows, 2, n, rows, 2 * half), jnp.bfloat16),
        pltpu.VMEM((n, rows, 2, rows, half), jnp.bfloat16),
    ]
    sems = [dma((count, n)), dma((count, n)), dma((count, n)), dma((count, n)), dma((2, count))]
    if first:
        operands = (send, speeds, stat_in) + tables
        in_specs = [hbm, hbm, vmem] + [vmem] * 4
        out_shape += [
            jax.ShapeDtypeStruct((3, rows, m, length // m, length), jnp.bfloat16),
            jax.ShapeDtypeStruct((n, 8, 128), jnp.float32),
        ]
        scratch += [pltpu.VMEM((8, length), jnp.float32), pltpu.VMEM((8, 128), jnp.float32)]
        sems += [dma((count, m)), dma((count, m)), dma((count,)), dma((n,)), dma((n,)), dma]
    else:
        operands = (send, speeds) + tables
        in_specs = [hbm, vmem] + [vmem] * 4
    return pl.pallas_call(
        functools.partial(stage_kernel, n, m, rows, chunk, band, first),
        out_shape=out_shape,
        in_specs=in_specs,
        out_specs=[vmem] * len(out_shape),
        scratch_shapes=scratch + sems,
        compiler_params=pltpu.CompilerParams(
            collective_id=0 if first else 1,
            has_side_effects=True,
            vmem_limit_bytes=56 * 1024 * 1024,
        ),
        name="stage_one" if first else "stage_two",
    )(*operands)


def body(n, m, scalar_state, velocity, species, kappa_table, dealias_bound):
    rows = scalar_state.shape[2]
    length = scalar_state.shape[3]
    half = length // 2
    total_count = kappa_table.shape[0]
    full_cos, full_sin, inv_cos, inv_sin, fwd_cos, fwd_sin = build_tables(length)
    inv_y = jnp.concatenate(
        [jnp.concatenate([full_cos, -full_sin], axis=1), jnp.concatenate([full_sin, full_cos], axis=1)], axis=0
    )
    fwd_y = inv_y.T
    inv_x = jnp.concatenate([inv_cos, -inv_sin], axis=0)
    fwd_x = jnp.concatenate([fwd_cos, -fwd_sin], axis=1)
    inv_z = inv_y.reshape(2, length, 2 * length).transpose(1, 0, 2).reshape(2 * length, 2 * length)
    fwd_z = fwd_y.reshape(2 * length, 2, length).transpose(0, 2, 1).reshape(2, length, 2 * length)
    tables = (inv_y, inv_x, fwd_x, fwd_y)
    ky_index = lax.axis_index("fft") * rows + jnp.arange(rows, dtype=jnp.int32)
    ky_wave = jnp.where(ky_index < half, ky_index, ky_index - length).astype(jnp.float32)[:, None, None]
    kz_index = jnp.arange(length, dtype=jnp.int32)
    kz_wave = jnp.where(kz_index < half, kz_index, kz_index - length).astype(jnp.float32)[None, :, None]
    kx_wave = jnp.arange(half, dtype=jnp.int32).astype(jnp.float32)[None, None, :]
    ksquare = kx_wave * kx_wave + ky_wave * ky_wave + kz_wave * kz_wave
    weight = jnp.where(kx_wave == 0.0, 1.0, 2.0).astype(jnp.float32)
    cell_count = float(length) ** 3
    step_size = cfl_number * 2.0 * math.pi / length

    def z_inverse(real_part, imag_part):
        plain = jnp.concatenate([real_part, imag_part], axis=1)
        deriv = jnp.concatenate([-kz_wave * imag_part, kz_wave * real_part], axis=1)
        both = jnp.concatenate([plain, deriv], axis=2).astype(jnp.bfloat16)
        result = jnp.einsum("ab,ybx->ayx", inv_z, both, preferred_element_type=jnp.float32)
        return result.astype(jnp.bfloat16).reshape(n, rows, 2, rows, 2 * half)

    def z_forward(pieces, bound):
        result = jnp.einsum(
            "rkb,byx->rykx",
            fwd_z,
            pieces.reshape(2 * length, rows, half),
            preferred_element_type=jnp.float32,
        )
        keep = ksquare <= bound * bound
        return jnp.where(keep, -result[0], 0.0), jnp.where(keep, -result[1], 0.0)

    start_real = scalar_state[0, 0]
    start_imag = scalar_state[0, 1]
    bound = dealias_bound[0].astype(jnp.float32)
    energy = weight * (start_real * start_real + start_imag * start_imag)
    local_var = jnp.sum(energy) / cell_count
    local_grad = jnp.sum(ksquare * energy) / cell_count
    line = jnp.arange(8, dtype=jnp.int32)[:, None]
    stat_in = jnp.broadcast_to(jnp.where(line == 0, local_var, local_grad), (8, 128))
    pieces, speeds, stats = run_stage(
        n, m, rows, True, z_inverse(start_real, start_imag), velocity, tables, stat_in
    )
    variance = jnp.sum(stats[:, 0, 0])
    mean_grad = jnp.sum(stats[:, 1, 0])
    peak_value = jnp.max(stats[:, 2, 0])
    matches = species[0] == jnp.arange(total_count, dtype=jnp.int32)
    base_kappa = jnp.sum(jnp.where(matches, kappa_table, 0.0))
    kappa = base_kappa * peak_value * jnp.sqrt(variance) / (mean_grad + 1e-06)
    factor = jnp.exp(-kappa * ksquare * step_size)
    first_real, first_imag = z_forward(pieces, bound)
    mid_real = factor * (start_real + step_size * first_real)
    mid_imag = factor * (start_imag + step_size * first_imag)
    (again,) = run_stage(n, m, rows, False, z_inverse(mid_real, mid_imag), speeds, tables)
    second_real, second_imag = z_forward(again, bound)
    new_real = factor * start_real + 0.5 * step_size * (factor * first_real + second_real)
    new_imag = factor * start_imag + 0.5 * step_size * (factor * first_imag + second_imag)
    return (jnp.stack([new_real, new_imag])[None], kappa[None])


def solution(mesh):
    placed = (
        P("scal", None, "fft", None, None),
        P(None, "fft", "scal", None),
        P("scal"),
        P(),
        P("scal"),
    )
    return jax.shard_map(
        functools.partial(body, mesh.shape["fft"], mesh.shape["scal"]),
        mesh=mesh,
        in_specs=placed,
        out_specs=(P("scal", None, "fft", None, None), P("scal")),
        check_vma=False,
    )
```

```python
import functools
import math

import numpy as np

import jax
import jax.numpy as jnp
from jax import lax
from jax.experimental import pallas as pl
from jax.experimental.pallas import tpu as pltpu
from jax.sharding import PartitionSpec as P

MESH = pl.DeviceIdType.MESH
cfl_number = 0.2


def twiddle(size_in, size_out, length):
    row_index = np.arange(size_in, dtype=np.int32)[:, None]
    col_index = np.arange(size_out, dtype=np.int32)[None, :]
    angles = (row_index * col_index % length).astype(np.float32) * np.float32(2.0 * math.pi / length)
    norming = np.float32(1.0 / math.sqrt(length))
    return (np.cos(angles) * norming, np.sin(angles) * norming)


def build_tables(length):
    half = length // 2
    quarter = half // 4
    full_cos, full_sin = twiddle(length, length, length)
    inv_cos, inv_sin = twiddle(half, length, length)
    weight = np.where(np.arange(half) == 0, 1.0, 2.0).astype(np.float32)[:, None]
    fwd_cos, fwd_sin = twiddle(length, half, length)
    inv_y = np.block([[full_cos, -full_sin], [full_sin, full_cos]])
    inv_x = np.concatenate([inv_cos * weight, -inv_sin * weight], axis=0)
    orders = [
        np.concatenate([((p - l - 1) % 4) * quarter + np.arange(quarter) for l in range(4)]) for p in range(4)
    ]
    fwd_x = np.stack([np.concatenate([fwd_cos[:, o], -fwd_sin[:, o]], axis=1) for o in orders])
    return tuple(jnp.asarray(t.astype(np.float32).astype(jnp.bfloat16)) for t in (inv_y, inv_x, fwd_x))


def dot(a, b):
    return jnp.dot(a, b, preferred_element_type=jnp.float32)


def stage_kernel(n, m, rows, chunk, band, first, *refs):
    if first:
        (send, vel, stat_in, inv_y, inv_x, fwd_x, fwd_y,
         gout, uall, stat_out,
         recv, fsend, raw, packed, peak, stat, s_send, s_recv, f_send, f_recv, l_sem, u_send, u_recv, u_loc,
         t_send, t_recv, t_loc) = refs
    else:
        (send, uall, inv_y, inv_x, fwd_x, fwd_y,
         gout,
         recv, fsend, raw, packed, s_send, s_recv, f_send, f_recv, l_sem) = refs
    length = n * rows
    half = length // 2
    count = rows // chunk
    me = lax.axis_index("fft")
    mine = lax.axis_index("scal")

    groups = rows // 4
    quarter = half // 4

    def needed(d, t):
        low = d * rows
        least = jnp.where(low < half, low, length - low - rows + 1)
        return (t * quarter) ** 2 + least * least <= band * band

    def by_tiles(d, act):
        for k in range(1, 4):
            wanted = needed(d, k - 1)
            if k < 3:
                wanted = jnp.logical_and(wanted, jnp.logical_not(needed(d, k)))

            @pl.when(wanted)
            def _():
                act(k)

    barrier = pltpu.get_barrier_semaphore()

    def greet(j, carry):
        pl.semaphore_signal(barrier, inc=1, device_id={"fft": lax.rem(me + j, n)}, device_id_type=MESH)
        return carry

    lax.fori_loop(1, n, greet, 0)
    if first:
        def greet_other(j, carry):
            pl.semaphore_signal(
                barrier, inc=1, device_id={"scal": lax.rem(mine + j, m)}, device_id_type=MESH
            )
            return carry

        lax.fori_loop(1, m, greet_other, 0)
        pl.semaphore_wait(barrier, n + m - 2)
    else:
        pl.semaphore_wait(barrier, n - 1)

    def inverse_copy(c, d, slot):
        return pltpu.make_async_remote_copy(
            src_ref=send.at[:, d, pl.ds(c * chunk, chunk)],
            dst_ref=recv.at[:, pl.ds(c * chunk, chunk), slot],
            send_sem=s_send.at[c, d],
            recv_sem=s_recv.at[c, slot],
            device_id={"fft": d},
            device_id_type=MESH,
        )

    def own_copy(c):
        return pltpu.make_async_copy(
            send.at[:, me, pl.ds(c * chunk, chunk)], recv.at[:, pl.ds(c * chunk, chunk), me], l_sem.at[0, c]
        )

    def speed_copy(c, s, slot):
        return pltpu.make_async_remote_copy(
            src_ref=vel.at[:, pl.ds(c * chunk, chunk)],
            dst_ref=uall.at[:, pl.ds(c * chunk, chunk), slot],
            send_sem=u_send.at[c, s],
            recv_sem=u_recv.at[c, slot],
            device_id={"scal": s},
            device_id_type=MESH,
        )

    def own_speed(c):
        return pltpu.make_async_copy(
            vel.at[:, pl.ds(c * chunk, chunk)], uall.at[:, pl.ds(c * chunk, chunk), mine], u_loc.at[c]
        )

    def forward_copy(g, d, slot, k):
        return pltpu.make_async_remote_copy(
            src_ref=fsend.at[d, g, pl.ds(0, k)],
            dst_ref=raw.at[slot, g, pl.ds(0, k)],
            send_sem=f_send.at[g, d],
            recv_sem=f_recv.at[g, slot],
            device_id={"fft": d},
            device_id_type=MESH,
        )

    def own_forward(g):
        return pltpu.make_async_copy(fsend.at[me, g], raw.at[me, g], l_sem.at[1, g])

    def stat_copy(d, slot):
        return pltpu.make_async_remote_copy(
            src_ref=stat,
            dst_ref=stat_out.at[slot],
            send_sem=t_send.at[d],
            recv_sem=t_recv.at[slot],
            device_id={"fft": d},
            device_id_type=MESH,
        )

    def start_chunk(c, carry):
        def one(j, inner):
            inverse_copy(c, lax.rem(me + j, n), me).start()
            return inner

        lax.fori_loop(1, n, one, 0)
        own_copy(c).start()
        if first:
            def two(j, inner):
                speed_copy(c, lax.rem(mine + j, m), mine).start()
                return inner

            lax.fori_loop(1, m, two, 0)
            own_speed(c).start()
        return carry

    lax.fori_loop(0, count, start_chunk, 0)

    if first:
        peak[...] = jnp.zeros_like(peak)

    for t in range(3):
        @pl.when(jnp.logical_not(needed(me, t)))
        def _():
            def clear(j, carry):
                raw[lax.rem(me + j, n), :, t] = jnp.zeros((groups, 2, rows, half), jnp.bfloat16)
                return carry

            lax.fori_loop(1, n, clear, 0)

    row = lax.broadcasted_iota(jnp.int32, (length, half), 0)
    ky = jnp.where(row < half, row, row - length).astype(jnp.float32)
    kx = lax.broadcasted_iota(jnp.int32, (length, half), 1).astype(jnp.float32)

    lane = lax.broadcasted_iota(jnp.int32, (2 * length, half), 1) // quarter

    def pick(choices):
        result = choices[-1]
        for i in range(len(choices) - 2, -1, -1):
            result = jnp.where(lane == i, choices[i], result)
        return result

    def pair(z, h):
        parts = []
        for p in range(2):
            block = jnp.concatenate([recv[q, z + p].reshape(length, 2 * half) for q in range(2)], axis=0)
            w_real = block[:length, :half].astype(jnp.float32)
            w_imag = block[length:, :half].astype(jnp.float32)
            turned = jnp.concatenate(
                [(-ky * w_imag).astype(jnp.bfloat16), (ky * w_real).astype(jnp.bfloat16)], axis=0
            )
            parts += [block, turned]
        section = dot(inv_y[...], jnp.concatenate(parts, axis=1))
        halves = []
        for p in range(2):
            at = 3 * half * p
            w_real = section[:length, at : at + half]
            w_imag = section[length:, at : at + half]
            sides = [
                (-kx * w_imag, kx * w_real),
                (section[:length, at + 2 * half : at + 3 * half], section[length:, at + 2 * half : at + 3 * half]),
                (section[:length, at + half : at + 2 * half], section[length:, at + half : at + 2 * half]),
            ]
            total = None
            square = None
            for i, (re, im) in enumerate(sides):
                lhs = jnp.concatenate([re.astype(jnp.bfloat16), im.astype(jnp.bfloat16)], axis=1)
                grad = dot(lhs, inv_x[...])
                u = uall[i, z + p].reshape(length, length).astype(jnp.float32)
                total = u * grad if total is None else total + u * grad
                if first:
                    square = grad * grad if square is None else square + grad * grad
            if first:
                peak[...] = jnp.maximum(peak[...], jnp.max(square.reshape(length // 8, 8, length), axis=0))
            flat = dot(total.astype(jnp.bfloat16), fwd_x[2 * h + p]).astype(jnp.bfloat16)
            halves.append(jnp.concatenate([flat[:, :half], flat[:, half:]], axis=0))
        packed[h] = dot(fwd_y[...], jnp.concatenate(halves, axis=1))

    def run_group(g, carry):
        def one_pair(h, outer):
            c = 2 * g + h

            def arrive(j, inner):
                inverse_copy(c, lax.rem(me + j, n), lax.rem(me + n - j, n)).wait_recv()
                return inner

            lax.fori_loop(1, n, arrive, 0)
            own_copy(c).wait()
            if first:
                def arrive_speed(j, inner):
                    speed_copy(c, lax.rem(mine + j, m), lax.rem(mine + m - j, m)).wait_recv()
                    return inner

                lax.fori_loop(1, m, arrive_speed, 0)
                own_speed(c).wait()
            pair(c * chunk, h)
            return outer

        lax.fori_loop(0, 2, one_pair, 0)

        for t in range(3):
            chosen = [(i + 1 + t) % 4 for i in range(4)]
            tile = pick([packed[p // 2, :, (p % 2) * half : (p % 2 + 1) * half] for p in chosen])
            tile = tile.astype(jnp.bfloat16)
            for q in range(2):
                fsend[:, g, t, q] = tile[q * length : (q + 1) * length].reshape(n, rows, half)

        def leave(j, inner):
            d = lax.rem(me + j, n)
            by_tiles(d, lambda k: forward_copy(g, d, me, k).start())
            return inner

        lax.fori_loop(1, n, leave, 0)
        own_forward(g).start()
        return carry

    lax.fori_loop(0, groups, run_group, 0)

    if first:
        line = lax.broadcasted_iota(jnp.int32, stat.shape, 0)
        largest = jnp.sqrt(jnp.max(peak[...], keepdims=True))
        stat[...] = jnp.where(line == 2, largest, stat_in[...])

        def tell(j, carry):
            stat_copy(lax.rem(me + j, n), me).start()
            return carry

        lax.fori_loop(1, n, tell, 0)
        pltpu.make_async_copy(stat, stat_out.at[me], t_loc).start()

    def unpack(g, carry):
        def one(j, inner):
            d = lax.rem(me + j, n)
            by_tiles(me, lambda k: forward_copy(g, d, lax.rem(me + n - j, n), k).wait_recv())
            return inner

        lax.fori_loop(1, n, one, 0)
        own_forward(g).wait()
        tiles = [raw[:, g, t].reshape(2 * length, half).astype(jnp.float32) for t in range(3)]
        for p in range(4):
            moved = [
                pltpu.roll(tiles[t], (2 * t + 1 - p) % 4 * quarter, 1) if (2 * t + 1 - p) % 4 else tiles[t]
                for t in range(3)
            ]
            plane = pick(moved + [jnp.zeros_like(tiles[0])]).astype(jnp.bfloat16).reshape(n, 2, rows, half)
            for q in range(2):
                gout[q, :, 4 * g + p] = plane[:, q]
        return carry

    lax.fori_loop(0, groups, unpack, 0)

    def finish(c, carry):
        def one(j, inner):
            inverse_copy(c, lax.rem(me + j, n), me).wait_send()
            return inner

        lax.fori_loop(1, n, one, 0)
        if first:
            def two(j, inner):
                speed_copy(c, lax.rem(mine + j, m), mine).wait_send()
                return inner

            lax.fori_loop(1, m, two, 0)
        return carry

    lax.fori_loop(0, count, finish, 0)

    def finish_forward(g, carry):
        def one(j, inner):
            d = lax.rem(me + j, n)
            by_tiles(d, lambda k: forward_copy(g, d, me, k).wait_send())
            return inner

        lax.fori_loop(1, n, one, 0)
        return carry

    lax.fori_loop(0, groups, finish_forward, 0)

    if first:
        def told(j, carry):
            stat_copy(lax.rem(me + j, n), me).wait_send()
            stat_copy(lax.rem(me + j, n), lax.rem(me + n - j, n)).wait_recv()
            return carry

        lax.fori_loop(1, n, told, 0)
        pltpu.make_async_copy(stat, stat_out.at[me], t_loc).wait()


def run_stage(n, m, rows, first, send, speeds, tables, stat_in=None):
    length = n * rows
    half = length // 2
    chunk = 2
    count = rows // chunk
    groups = rows // 4
    band = length // 3
    vmem = pl.BlockSpec(memory_space=pltpu.VMEM)
    hbm = pl.BlockSpec(memory_space=pl.ANY)
    dma = pltpu.SemaphoreType.DMA
    out_shape = [jax.ShapeDtypeStruct((2, n, rows, rows, half), jnp.bfloat16)]
    scratch = [
        pltpu.VMEM((2, rows, n, rows, 2 * half), jnp.bfloat16),
        pltpu.VMEM((n, groups, 3, 2, rows, half), jnp.bfloat16),
        pltpu.VMEM((n, groups, 3, 2, rows, half), jnp.bfloat16),
        pltpu.VMEM((2, 2 * length, 2 * half), jnp.float32),
    ]
    sems = [dma((count, n)), dma((count, n)), dma((groups, n)), dma((groups, n)), dma((2, count))]
    if first:
        operands = (send, speeds, stat_in) + tables
        in_specs = [hbm, hbm, vmem] + [vmem] * 4
        out_shape += [
            jax.ShapeDtypeStruct((3, rows, m, length // m, length), jnp.bfloat16),
            jax.ShapeDtypeStruct((n, 8, 128), jnp.float32),
        ]
        scratch += [pltpu.VMEM((8, length), jnp.float32), pltpu.VMEM((8, 128), jnp.float32)]
        sems += [dma((count, m)), dma((count, m)), dma((count,)), dma((n,)), dma((n,)), dma]
    else:
        operands = (send, speeds) + tables
        in_specs = [hbm, vmem] + [vmem] * 4
    return pl.pallas_call(
        functools.partial(stage_kernel, n, m, rows, chunk, band, first),
        out_shape=out_shape,
        in_specs=in_specs,
        out_specs=[vmem] * len(out_shape),
        scratch_shapes=scratch + sems,
        compiler_params=pltpu.CompilerParams(
            collective_id=0 if first else 1,
            has_side_effects=True,
            vmem_limit_bytes=56 * 1024 * 1024,
        ),
        name="stage_one" if first else "stage_two",
    )(*operands)


def body(n, m, scalar_state, velocity, species, kappa_table, dealias_bound):
    rows = scalar_state.shape[2]
    length = scalar_state.shape[3]
    half = length // 2
    total_count = kappa_table.shape[0]
    tables = build_tables(length)
    tables = lax.optimization_barrier(tables)
    inv_y = tables[0]
    fwd_y = jnp.concatenate(
        [
            jnp.concatenate([inv_y[:length, :length], inv_y[length:, :length]], axis=1),
            jnp.concatenate([inv_y[:length, length:], inv_y[:length, :length]], axis=1),
        ],
        axis=0,
    )
    tables = tables + (fwd_y,)
    ky_index = lax.axis_index("fft") * rows + jnp.arange(rows, dtype=jnp.int32)
    ky_wave = jnp.where(ky_index < half, ky_index, ky_index - length).astype(jnp.float32)[:, None, None]
    kz_index = jnp.arange(length, dtype=jnp.int32)
    kz_wave = jnp.where(kz_index < half, kz_index, kz_index - length).astype(jnp.float32)[None, :, None]
    kx_wave = jnp.arange(half, dtype=jnp.int32).astype(jnp.float32)[None, None, :]
    ksquare = kx_wave * kx_wave + ky_wave * ky_wave + kz_wave * kz_wave
    weight = jnp.where(kx_wave == 0.0, 1.0, 2.0).astype(jnp.float32)
    cell_count = float(length) ** 3
    step_size = cfl_number * 2.0 * math.pi / length

    def z_inverse(real_part, imag_part):
        plain = jnp.concatenate([real_part, imag_part], axis=1)
        deriv = jnp.concatenate([-kz_wave * imag_part, kz_wave * real_part], axis=1)
        both = jnp.concatenate([plain, deriv], axis=2).astype(jnp.bfloat16)
        result = jnp.einsum("ab,ybx->ayx", inv_y, both, preferred_element_type=jnp.float32)
        return result.astype(jnp.bfloat16).reshape(2, n, rows, rows, 2 * half)

    def z_forward(pieces, bound):
        result = jnp.einsum(
            "rkb,byx->rykx",
            fwd_y.reshape(2, length, 2 * length),
            pieces.reshape(2 * length, rows, half),
            preferred_element_type=jnp.float32,
        )
        keep = ksquare <= bound * bound
        return jnp.where(keep, -result[0], 0.0), jnp.where(keep, -result[1], 0.0)

    start_real = scalar_state[0, 0]
    start_imag = scalar_state[0, 1]
    bound = dealias_bound[0].astype(jnp.float32)
    energy = weight * (start_real * start_real + start_imag * start_imag)
    local_var = jnp.sum(energy) / cell_count
    local_grad = jnp.sum(ksquare * energy) / cell_count
    line = jnp.arange(8, dtype=jnp.int32)[:, None]
    stat_in = jnp.broadcast_to(jnp.where(line == 0, local_var, local_grad), (8, 128))
    pieces, speeds, stats = run_stage(
        n, m, rows, True, z_inverse(start_real, start_imag), velocity, tables, stat_in
    )
    variance = jnp.sum(stats[:, 0, 0])
    mean_grad = jnp.sum(stats[:, 1, 0])
    peak_value = jnp.max(stats[:, 2, 0])
    matches = species[0] == jnp.arange(total_count, dtype=jnp.int32)
    base_kappa = jnp.sum(jnp.where(matches, kappa_table, 0.0))
    kappa = base_kappa * peak_value * jnp.sqrt(variance) / (mean_grad + 1e-06)
    factor = jnp.exp(-kappa * ksquare * step_size)
    first_real, first_imag = z_forward(pieces, bound)
    mid_real = factor * (start_real + step_size * first_real)
    mid_imag = factor * (start_imag + step_size * first_imag)
    (again,) = run_stage(n, m, rows, False, z_inverse(mid_real, mid_imag), speeds, tables)
    second_real, second_imag = z_forward(again, bound)
    new_real = factor * start_real + 0.5 * step_size * (factor * first_real + second_real)
    new_imag = factor * start_imag + 0.5 * step_size * (factor * first_imag + second_imag)
    return (jnp.stack([new_real, new_imag])[None], kappa[None])


def solution(mesh):
    placed = (
        P("scal", None, "fft", None, None),
        P(None, "fft", "scal", None),
        P("scal"),
        P(),
        P("scal"),
    )
    return jax.shard_map(
        functools.partial(body, mesh.shape["fft"], mesh.shape["scal"]),
        mesh=mesh,
        in_specs=placed,
        out_specs=(P("scal", None, "fft", None, None), P("scal")),
        check_vma=False,
    )
```

```python
import functools
import math

import numpy as np

import jax
import jax.numpy as jnp
from jax import lax
from jax.experimental import pallas as pl
from jax.experimental.pallas import tpu as pltpu
from jax.sharding import PartitionSpec as P

MESH = pl.DeviceIdType.MESH
cfl_number = 0.2


def twiddle(size_in, size_out, length):
    row_index = np.arange(size_in, dtype=np.int32)[:, None]
    col_index = np.arange(size_out, dtype=np.int32)[None, :]
    angles = (row_index * col_index % length).astype(np.float32) * np.float32(2.0 * math.pi / length)
    norming = np.float32(1.0 / math.sqrt(length))
    return (np.cos(angles) * norming, np.sin(angles) * norming)


def build_tables(length):
    half = length // 2
    quarter = half // 4
    full_cos, full_sin = twiddle(length, length, length)
    inv_cos, inv_sin = twiddle(half, length, length)
    weight = np.where(np.arange(half) == 0, 1.0, 2.0).astype(np.float32)[:, None]
    fwd_cos, fwd_sin = twiddle(length, half, length)
    inv_y = np.block([[full_cos, -full_sin], [full_sin, full_cos]])
    inv_x = np.concatenate([inv_cos * weight, -inv_sin * weight], axis=0)
    orders = [
        np.concatenate([((p - l - 1) % 4) * quarter + np.arange(quarter) for l in range(4)]) for p in range(4)
    ]
    fwd_x = np.stack([np.concatenate([fwd_cos[:, o], -fwd_sin[:, o]], axis=1) for o in orders])
    return tuple(jnp.asarray(t.astype(np.float32).astype(jnp.bfloat16)) for t in (inv_y, inv_x, fwd_x))


def dot(a, b):
    return jnp.dot(a, b, preferred_element_type=jnp.float32)


def stage_kernel(n, m, rows, chunk, band, first, *refs):
    if first:
        (send, vel, stat_in, inv_y, inv_x, fwd_x, fwd_y,
         gout, uall, stat_out,
         recv, fsend, raw, packed, peak, stat, s_send, s_recv, f_send, f_recv, l_sem, u_send, u_recv, u_loc,
         t_send, t_recv, t_loc) = refs
    else:
        (send, uall, inv_y, inv_x, fwd_x, fwd_y,
         gout,
         recv, fsend, raw, packed, s_send, s_recv, f_send, f_recv, l_sem) = refs
    length = n * rows
    half = length // 2
    count = rows // chunk
    me = lax.axis_index("fft")
    mine = lax.axis_index("scal")

    groups = rows // 4
    quarter = half // 4

    def needed(d, t):
        low = d * rows
        least = jnp.where(low < half, low, length - low - rows + 1)
        return (t * quarter) ** 2 + least * least <= band * band

    def by_tiles(d, act):
        for k in range(1, 4):
            wanted = needed(d, k - 1)
            if k < 3:
                wanted = jnp.logical_and(wanted, jnp.logical_not(needed(d, k)))

            @pl.when(wanted)
            def _():
                act(k)

    barrier = pltpu.get_barrier_semaphore()

    def greet(j, carry):
        pl.semaphore_signal(barrier, inc=1, device_id={"fft": lax.rem(me + j, n)}, device_id_type=MESH)
        return carry

    lax.fori_loop(1, n, greet, 0)
    if first:
        def greet_other(j, carry):
            pl.semaphore_signal(
                barrier, inc=1, device_id={"scal": lax.rem(mine + j, m)}, device_id_type=MESH
            )
            return carry

        lax.fori_loop(1, m, greet_other, 0)
        pl.semaphore_wait(barrier, n + m - 2)
    else:
        pl.semaphore_wait(barrier, n - 1)

    def inverse_copy(c, d, slot):
        return pltpu.make_async_remote_copy(
            src_ref=send.at[:, d, pl.ds(c * chunk, chunk)],
            dst_ref=recv.at[:, pl.ds(c * chunk, chunk), slot],
            send_sem=s_send.at[c, d],
            recv_sem=s_recv.at[c, slot],
            device_id={"fft": d},
            device_id_type=MESH,
        )

    def own_copy(c):
        return pltpu.make_async_copy(
            send.at[:, me, pl.ds(c * chunk, chunk)], recv.at[:, pl.ds(c * chunk, chunk), me], l_sem.at[0, c]
        )

    def speed_copy(c, s, slot):
        return pltpu.make_async_remote_copy(
            src_ref=vel.at[:, pl.ds(c * chunk, chunk)],
            dst_ref=uall.at[:, pl.ds(c * chunk, chunk), slot],
            send_sem=u_send.at[c, s],
            recv_sem=u_recv.at[c, slot],
            device_id={"scal": s},
            device_id_type=MESH,
        )

    def own_speed(c):
        return pltpu.make_async_copy(
            vel.at[:, pl.ds(c * chunk, chunk)], uall.at[:, pl.ds(c * chunk, chunk), mine], u_loc.at[c]
        )

    def forward_copy(g, d, slot, k):
        return pltpu.make_async_remote_copy(
            src_ref=fsend.at[d, g, pl.ds(0, k)],
            dst_ref=raw.at[slot, g, pl.ds(0, k)],
            send_sem=f_send.at[g, d],
            recv_sem=f_recv.at[g, slot],
            device_id={"fft": d},
            device_id_type=MESH,
        )

    def own_forward(g):
        return pltpu.make_async_copy(fsend.at[me, g], raw.at[me, g], l_sem.at[1, g])

    def stat_copy(d, slot):
        return pltpu.make_async_remote_copy(
            src_ref=stat,
            dst_ref=stat_out.at[slot],
            send_sem=t_send.at[d],
            recv_sem=t_recv.at[slot],
            device_id={"fft": d},
            device_id_type=MESH,
        )

    def start_chunk(c, carry):
        def one(j, inner):
            inverse_copy(c, lax.rem(me + j, n), me).start()
            return inner

        lax.fori_loop(1, n, one, 0)
        own_copy(c).start()
        if first:
            def two(j, inner):
                speed_copy(c, lax.rem(mine + j, m), mine).start()
                return inner

            lax.fori_loop(1, m, two, 0)
            own_speed(c).start()
        return carry

    lax.fori_loop(0, count, start_chunk, 0)

    if first:
        peak[...] = jnp.zeros_like(peak)

    for t in range(3):
        @pl.when(jnp.logical_not(needed(me, t)))
        def _():
            def clear(j, carry):
                raw[lax.rem(me + j, n), :, t] = jnp.zeros((groups, 2, rows, half), jnp.bfloat16)
                return carry

            lax.fori_loop(1, n, clear, 0)

    row = lax.broadcasted_iota(jnp.int32, (length, half), 0)
    ky = jnp.where(row < half, row, row - length).astype(jnp.float32)
    kx = lax.broadcasted_iota(jnp.int32, (length, half), 1).astype(jnp.float32)

    lane = lax.broadcasted_iota(jnp.int32, (2 * length, half), 1) // quarter

    def pick(choices):
        result = choices[-1]
        for i in range(len(choices) - 2, -1, -1):
            result = jnp.where(lane == i, choices[i], result)
        return result

    def pair(z, h):
        parts = []
        for p in range(2):
            block = jnp.concatenate([recv[q, z + p].reshape(length, 2 * half) for q in range(2)], axis=0)
            w_real = block[:length, :half].astype(jnp.float32)
            w_imag = block[length:, :half].astype(jnp.float32)
            turned = jnp.concatenate(
                [(-ky * w_imag).astype(jnp.bfloat16), (ky * w_real).astype(jnp.bfloat16)], axis=0
            )
            parts += [block, turned]
        section = dot(inv_y[...], jnp.concatenate(parts, axis=1))
        halves = []
        for p in range(2):
            at = 3 * half * p
            w_real = section[:length, at : at + half]
            w_imag = section[length:, at : at + half]
            sides = [
                (-kx * w_imag, kx * w_real),
                (section[:length, at + 2 * half : at + 3 * half], section[length:, at + 2 * half : at + 3 * half]),
                (section[:length, at + half : at + 2 * half], section[length:, at + half : at + 2 * half]),
            ]
            total = None
            square = None
            for i, (re, im) in enumerate(sides):
                lhs = jnp.concatenate([re.astype(jnp.bfloat16), im.astype(jnp.bfloat16)], axis=1)
                grad = dot(lhs, inv_x[...])
                u = uall[i, z + p].reshape(length, length).astype(jnp.float32)
                total = u * grad if total is None else total + u * grad
                if first:
                    square = grad * grad if square is None else square + grad * grad
            if first:
                peak[...] = jnp.maximum(peak[...], jnp.max(square.reshape(length // 8, 8, length), axis=0))
            flat = dot(total.astype(jnp.bfloat16), fwd_x[2 * h + p]).astype(jnp.bfloat16)
            halves.append(jnp.concatenate([flat[:, :half], flat[:, half:]], axis=0))
        packed[h] = dot(fwd_y[...], jnp.concatenate(halves, axis=1))

    def unpack(g):
        def one(j, inner):
            d = lax.rem(me + j, n)
            by_tiles(me, lambda k: forward_copy(g, d, lax.rem(me + n - j, n), k).wait_recv())
            return inner

        lax.fori_loop(1, n, one, 0)
        own_forward(g).wait()
        tiles = [raw[:, g, t].reshape(2 * length, half).astype(jnp.float32) for t in range(3)]
        for p in range(4):
            moved = [
                pltpu.roll(tiles[t], (2 * t + 1 - p) % 4 * quarter, 1) if (2 * t + 1 - p) % 4 else tiles[t]
                for t in range(3)
            ]
            plane = pick(moved + [jnp.zeros_like(tiles[0])]).astype(jnp.bfloat16).reshape(n, 2, rows, half)
            for q in range(2):
                gout[q, :, 4 * g + p] = plane[:, q]

    def run_group(g, carry):
        def one_pair(h, outer):
            c = 2 * g + h

            def arrive(j, inner):
                inverse_copy(c, lax.rem(me + j, n), lax.rem(me + n - j, n)).wait_recv()
                return inner

            lax.fori_loop(1, n, arrive, 0)
            own_copy(c).wait()
            if first:
                def arrive_speed(j, inner):
                    speed_copy(c, lax.rem(mine + j, m), lax.rem(mine + m - j, m)).wait_recv()
                    return inner

                lax.fori_loop(1, m, arrive_speed, 0)
                own_speed(c).wait()
            pair(c * chunk, h)
            return outer

        lax.fori_loop(0, 2, one_pair, 0)

        for t in range(3):
            chosen = [(i + 1 + t) % 4 for i in range(4)]
            tile = pick([packed[p // 2, :, (p % 2) * half : (p % 2 + 1) * half] for p in chosen])
            tile = tile.astype(jnp.bfloat16)
            for q in range(2):
                fsend[:, g, t, q] = tile[q * length : (q + 1) * length].reshape(n, rows, half)

        def leave(j, inner):
            d = lax.rem(me + j, n)
            by_tiles(d, lambda k: forward_copy(g, d, me, k).start())
            return inner

        lax.fori_loop(1, n, leave, 0)
        own_forward(g).start()

        @pl.when(g >= 1)
        def _():
            unpack(g - 1)

        return carry

    lax.fori_loop(0, groups, run_group, 0)

    if first:
        line = lax.broadcasted_iota(jnp.int32, stat.shape, 0)
        largest = jnp.sqrt(jnp.max(peak[...], keepdims=True))
        stat[...] = jnp.where(line == 2, largest, stat_in[...])

        def tell(j, carry):
            stat_copy(lax.rem(me + j, n), me).start()
            return carry

        lax.fori_loop(1, n, tell, 0)
        pltpu.make_async_copy(stat, stat_out.at[me], t_loc).start()

    unpack(groups - 1)

    def finish(c, carry):
        def one(j, inner):
            inverse_copy(c, lax.rem(me + j, n), me).wait_send()
            return inner

        lax.fori_loop(1, n, one, 0)
        if first:
            def two(j, inner):
                speed_copy(c, lax.rem(mine + j, m), mine).wait_send()
                return inner

            lax.fori_loop(1, m, two, 0)
        return carry

    lax.fori_loop(0, count, finish, 0)

    def finish_forward(g, carry):
        def one(j, inner):
            d = lax.rem(me + j, n)
            by_tiles(d, lambda k: forward_copy(g, d, me, k).wait_send())
            return inner

        lax.fori_loop(1, n, one, 0)
        return carry

    lax.fori_loop(0, groups, finish_forward, 0)

    if first:
        def told(j, carry):
            stat_copy(lax.rem(me + j, n), me).wait_send()
            stat_copy(lax.rem(me + j, n), lax.rem(me + n - j, n)).wait_recv()
            return carry

        lax.fori_loop(1, n, told, 0)
        pltpu.make_async_copy(stat, stat_out.at[me], t_loc).wait()


def run_stage(n, m, rows, first, send, speeds, tables, stat_in=None):
    length = n * rows
    half = length // 2
    chunk = 2
    count = rows // chunk
    groups = rows // 4
    band = length // 3
    vmem = pl.BlockSpec(memory_space=pltpu.VMEM)
    hbm = pl.BlockSpec(memory_space=pl.ANY)
    dma = pltpu.SemaphoreType.DMA
    out_shape = [jax.ShapeDtypeStruct((2, n, rows, rows, half), jnp.bfloat16)]
    scratch = [
        pltpu.VMEM((2, rows, n, rows, 2 * half), jnp.bfloat16),
        pltpu.VMEM((n, groups, 3, 2, rows, half), jnp.bfloat16),
        pltpu.VMEM((n, groups, 3, 2, rows, half), jnp.bfloat16),
        pltpu.VMEM((2, 2 * length, 2 * half), jnp.float32),
    ]
    sems = [dma((count, n)), dma((count, n)), dma((groups, n)), dma((groups, n)), dma((2, count))]
    if first:
        operands = (send, speeds, stat_in) + tables
        in_specs = [hbm, hbm, vmem] + [vmem] * 4
        out_shape += [
            jax.ShapeDtypeStruct((3, rows, m, length // m, length), jnp.bfloat16),
            jax.ShapeDtypeStruct((n, 8, 128), jnp.float32),
        ]
        scratch += [pltpu.VMEM((8, length), jnp.float32), pltpu.VMEM((8, 128), jnp.float32)]
        sems += [dma((count, m)), dma((count, m)), dma((count,)), dma((n,)), dma((n,)), dma]
    else:
        operands = (send, speeds) + tables
        in_specs = [hbm, vmem] + [vmem] * 4
    return pl.pallas_call(
        functools.partial(stage_kernel, n, m, rows, chunk, band, first),
        out_shape=out_shape,
        in_specs=in_specs,
        out_specs=[vmem] * len(out_shape),
        scratch_shapes=scratch + sems,
        compiler_params=pltpu.CompilerParams(
            collective_id=0 if first else 1,
            has_side_effects=True,
            vmem_limit_bytes=56 * 1024 * 1024,
        ),
        name="stage_one" if first else "stage_two",
    )(*operands)


def body(n, m, scalar_state, velocity, species, kappa_table, dealias_bound):
    rows = scalar_state.shape[2]
    length = scalar_state.shape[3]
    half = length // 2
    total_count = kappa_table.shape[0]
    tables = build_tables(length)
    tables = lax.optimization_barrier(tables)
    inv_y = tables[0]
    fwd_y = jnp.concatenate(
        [
            jnp.concatenate([inv_y[:length, :length], inv_y[length:, :length]], axis=1),
            jnp.concatenate([inv_y[:length, length:], inv_y[:length, :length]], axis=1),
        ],
        axis=0,
    )
    tables = tables + (fwd_y,)
    ky_index = lax.axis_index("fft") * rows + jnp.arange(rows, dtype=jnp.int32)
    ky_wave = jnp.where(ky_index < half, ky_index, ky_index - length).astype(jnp.float32)[:, None, None]
    kz_index = jnp.arange(length, dtype=jnp.int32)
    kz_wave = jnp.where(kz_index < half, kz_index, kz_index - length).astype(jnp.float32)[None, :, None]
    kx_wave = jnp.arange(half, dtype=jnp.int32).astype(jnp.float32)[None, None, :]
    ksquare = kx_wave * kx_wave + ky_wave * ky_wave + kz_wave * kz_wave
    weight = jnp.where(kx_wave == 0.0, 1.0, 2.0).astype(jnp.float32)
    cell_count = float(length) ** 3
    step_size = cfl_number * 2.0 * math.pi / length

    def z_inverse(real_part, imag_part):
        plain = jnp.concatenate([real_part, imag_part], axis=1)
        deriv = jnp.concatenate([-kz_wave * imag_part, kz_wave * real_part], axis=1)
        both = jnp.concatenate([plain, deriv], axis=2).astype(jnp.bfloat16)
        result = jnp.einsum("ab,ybx->ayx", inv_y, both, preferred_element_type=jnp.float32)
        return result.astype(jnp.bfloat16).reshape(2, n, rows, rows, 2 * half)

    def z_forward(pieces, bound):
        result = jnp.einsum(
            "rkb,byx->rykx",
            fwd_y.reshape(2, length, 2 * length),
            pieces.reshape(2 * length, rows, half),
            preferred_element_type=jnp.float32,
        )
        keep = ksquare <= bound * bound
        return jnp.where(keep[None], -result, 0.0)

    start_real = scalar_state[0, 0]
    start_imag = scalar_state[0, 1]
    bound = dealias_bound[0].astype(jnp.float32)
    energy = weight * (start_real * start_real + start_imag * start_imag)
    local_var = jnp.sum(energy) / cell_count
    local_grad = jnp.sum(ksquare * energy) / cell_count
    line = jnp.arange(8, dtype=jnp.int32)[:, None]
    stat_in = jnp.broadcast_to(jnp.where(line == 0, local_var, local_grad), (8, 128))
    pieces, speeds, stats = run_stage(
        n, m, rows, True, z_inverse(start_real, start_imag), velocity, tables, stat_in
    )
    variance = jnp.sum(stats[:, 0, 0])
    mean_grad = jnp.sum(stats[:, 1, 0])
    peak_value = jnp.max(stats[:, 2, 0])
    matches = species[0] == jnp.arange(total_count, dtype=jnp.int32)
    base_kappa = jnp.sum(jnp.where(matches, kappa_table, 0.0))
    kappa = base_kappa * peak_value * jnp.sqrt(variance) / (mean_grad + 1e-06)
    factor = jnp.exp(-kappa * ksquare * step_size)
    start = scalar_state[0]
    first = z_forward(pieces, bound)
    middle = factor[None] * (start + step_size * first)
    (again,) = run_stage(n, m, rows, False, z_inverse(middle[0], middle[1]), speeds, tables)
    second = z_forward(again, bound)
    updated = factor[None] * start + 0.5 * step_size * (factor[None] * first + second)
    return (updated[None], kappa[None])


def solution(mesh):
    placed = (
        P("scal", None, "fft", None, None),
        P(None, "fft", "scal", None),
        P("scal"),
        P(),
        P("scal"),
    )
    return jax.shard_map(
        functools.partial(body, mesh.shape["fft"], mesh.shape["scal"]),
        mesh=mesh,
        in_specs=placed,
        out_specs=(P("scal", None, "fft", None, None), P("scal")),
        check_vma=False,
    )
```
